64 devices in a mesh: dp: 8 (over x, y, core), tp: 8 (over z).
Axes of the slice: x: 2, y: 2, z: 8, core: 2. Of those that a mesh axis runs over, the one named last changes fastest.
The devices are a block of a 4x4x8 slice.
Arguments:
- x: bfloat16 [1024, 5120], P('dp'), parts along dimension 0
- w_gate: bfloat16 [5120, 27648], P(None, 'tp')
- w_up: bfloat16 [5120, 27648], P(None, 'tp')
- w_down: bfloat16 [27648, 5120], P('tp')
Outputs:
- output: bfloat16 [1024, 5120], P('dp'), parts along dimension 0
There are 8 independent parts. The reference program is written for one: setup_inputs(seed, part) draws one part's arguments, and reference() takes and returns one part's arrays. A program takes and returns all parts, laid end to end along the dimension named above; an argument that names none is the same for every part.
All inputs are finite; a program needn't handle non-finite values.
Results may differ from the reference program's by a relative error of at most 0.016.
Values are sent between devices in bfloat16 or wider.
A program may use at most 768 MiB of HBM per device.

```python
import jax
import jax.numpy as jnp

ROWS = 128
D = 5120
FF = 27648


def setup_inputs(seed: int = 0, part: int = 0) -> dict:
    kx, kg, ku, kd = jax.random.split(jax.random.key(seed), 4)
    drawn = {
        "x": jax.random.normal(jax.random.fold_in(kx, part), (ROWS, D), jnp.float32),
        "w_gate": jax.random.normal(kg, (D, FF), jnp.float32) * D**-0.5,
        "w_up": jax.random.normal(ku, (D, FF), jnp.float32) * D**-0.5,
        "w_down": jax.random.normal(kd, (FF, D), jnp.float32) * FF**-0.5,
    }
    return {k: v.astype(jnp.bfloat16) for k, v in drawn.items()}


def reference(x, w_gate, w_up, w_down):
    gate = jnp.dot(x, w_gate, preferred_element_type=jnp.float32)
    up = jnp.dot(x, w_up, preferred_element_type=jnp.float32)
    hidden = (jax.nn.silu(gate) * up).astype(jnp.bfloat16)
    return jnp.dot(hidden, w_down, preferred_element_type=jnp.float32).astype(jnp.bfloat16)
```

```python
import functools

import jax
import jax.numpy as jnp
from jax import lax
from jax.experimental import pallas as pl
from jax.experimental.pallas import tpu as pltpu
from jax.sharding import PartitionSpec as P

AXIS = "tp"
SLAB = 256
SLOTS = 3
CHUNKS = 4
LEFT, RIGHT = 0, 1


def kernel(n, x_hbm, g_hbm, u_hbm, d_hbm, out, xb, gb, ub, wd, hid, term, sbuf, rbuf,
           x_sem, g_sem, u_sem, d_sem, send_sem, rs_sem, ag_sem):
    rows, width = x_hbm.shape[0], d_hbm.shape[1] // n
    depth = g_hbm.shape[1]
    full, rest = depth // SLAB, depth % SLAB
    half = n // 2
    me = lax.axis_index(AXIS)
    near = {LEFT: lax.rem(me + n - 1, n), RIGHT: lax.rem(me + 1, n)}
    cr = rows // CHUNKS

    def at(offset):
        return lax.rem(me + offset + n, n)

    def slab(i, slot, size=SLAB):
        cols = pl.ds(pl.multiple_of(i * SLAB, 128), size)
        dst = (slot, slice(None), pl.ds(0, size))
        return (
            pltpu.make_async_copy(g_hbm.at[:, cols], gb.at[dst], g_sem.at[slot]),
            pltpu.make_async_copy(u_hbm.at[:, cols], ub.at[dst], u_sem.at[slot]),
        )

    order = [half]
    for k in range(half - 1, 0, -1):
        order += [-k, k]
    order += [0]
    place = {o: b for b, o in enumerate(order)}

    def down(b):
        cols = pl.ds(pl.multiple_of(at(order[b]) * width, 128), width)
        return pltpu.make_async_copy(d_hbm.at[:, cols], wd.at[b], d_sem.at[b])

    x_copy = pltpu.make_async_copy(x_hbm, xb, x_sem)
    x_copy.start()
    for i in range(min(SLOTS, full)):
        for c in slab(i, i):
            c.start()

    barrier = pltpu.get_barrier_semaphore()
    for side in (LEFT, RIGHT):
        pl.semaphore_signal(barrier, inc=1, device_id={AXIS: near[side]}, device_id_type=pl.DeviceIdType.MESH)

    x_copy.wait()

    def hidden(i, slot, size):
        for c in slab(i, slot, size):
            c.wait()
        x = xb[...]
        gate = jnp.dot(x, gb[slot, :, :size], preferred_element_type=jnp.float32)
        up = jnp.dot(x, ub[slot, :, :size], preferred_element_type=jnp.float32)
        cols = pl.ds(pl.multiple_of(i * SLAB, 128), size)
        hid[:, cols] = (jax.nn.silu(gate) * up).astype(jnp.bfloat16)

    @pl.loop(0, full)
    def _(i):
        slot = lax.rem(i, SLOTS)
        hidden(i, slot, SLAB)

        @pl.when(i + SLOTS < full)
        def _():
            for c in slab(i + SLOTS, slot):
                c.start()

        if rest:
            @pl.when(i + SLOTS == full)
            def _():
                for c in slab(full, full % SLOTS, rest):
                    c.start()
                down(0).start()

        for b in range(1, SLOTS):
            @pl.when(i + SLOTS == full + b)
            def _():
                down(b).start()

    for b in range(SLOTS, n):
        down(b).start()
    if rest:
        hidden(full, full % SLOTS, rest)

    def chunk(c):
        return pl.ds(c * cr, cr)

    def sum_copy(side, step, c):
        return pltpu.make_async_remote_copy(
            src_ref=sbuf.at[side, step, chunk(c)],
            dst_ref=rbuf.at[side, step, chunk(c)],
            send_sem=send_sem.at[0, side, step],
            recv_sem=rs_sem.at[side, step, c],
            device_id={AXIS: near[side]},
            device_id_type=pl.DeviceIdType.MESH,
        )

    def gather_copy(side, step, c):
        owner = at(step if side == LEFT else -step)
        ref = out.at[chunk(c), pl.ds(pl.multiple_of(owner * width, 128), width)]
        return pltpu.make_async_remote_copy(
            src_ref=ref,
            dst_ref=ref,
            send_sem=send_sem.at[1, side, step],
            recv_sem=ag_sem.at[side, step, c],
            device_id={AXIS: near[side]},
            device_id_type=pl.DeviceIdType.MESH,
        )

    def arrived(side, step, c):
        owner = at(step + 1 if side == LEFT else -step - 1)
        ref = out.at[chunk(c), pl.ds(pl.multiple_of(owner * width, 128), width)]
        pltpu.make_async_remote_copy(
            src_ref=ref, dst_ref=ref, send_sem=send_sem.at[1, side, step], recv_sem=ag_sem.at[side, step, c],
            device_id={AXIS: near[side]}, device_id_type=pl.DeviceIdType.MESH,
        ).wait_recv()

    low, high = tuple(range(CHUNKS // 2)), tuple(range(CHUNKS // 2, CHUNKS))
    first = {LEFT: low, RIGHT: high}

    def compute(offset):
        b = place[offset]
        down(b).wait()
        term[b] = jnp.dot(hid[...], wd[b], preferred_element_type=jnp.float32)

    def offset_of(side, step):
        return (-(half - step) if side == LEFT else half - step) if step else half

    def send_plain(side, step, c):
        b = place[offset_of(side, step)]
        sbuf[side, step, chunk(c)] = term[b, chunk(c)].astype(jnp.bfloat16)
        sum_copy(side, step, c).start()

    def send_sum(side, step, c):
        b = place[offset_of(side, step)]
        sum_copy(side, step - 1, c).wait_recv()
        total = term[b, chunk(c)] + rbuf[side, step - 1, chunk(c)].astype(jnp.float32)
        sbuf[side, step, chunk(c)] = total.astype(jnp.bfloat16)
        sum_copy(side, step, c).start()

    compute(half)
    pl.semaphore_wait(barrier, 2)
    for k in range(CHUNKS // 2):
        for side in (LEFT, RIGHT):
            send_plain(side, 0, first[side][k])
    last = {side: [c for c in range(CHUNKS) if c not in first[side]] for side in first}
    seq = {side: last[side] + list(first[side]) for side in first}
    for side in (LEFT, RIGHT):
        compute(offset_of(side, 1))
        for c in last[side]:
            send_plain(side, 1, c)
    for k in range(CHUNKS // 2):
        for side in (LEFT, RIGHT):
            send_sum(side, 1, first[side][k])
    for step in range(2, half):
        compute(offset_of(LEFT, step))
        send_sum(LEFT, step, seq[LEFT][0])
        compute(offset_of(RIGHT, step))
        send_sum(RIGHT, step, seq[RIGHT][0])
        for k in range(1, CHUNKS):
            for side in (LEFT, RIGHT):
                send_sum(side, step, seq[side][k])
    compute(0)

    mine = pl.ds(pl.multiple_of(me * width, 128), width)
    for c in range(CHUNKS):
        for side in (LEFT, RIGHT):
            sum_copy(side, half - 1, c).wait_recv()
        total = (
            term[place[0], chunk(c)]
            + rbuf[LEFT, half - 1, chunk(c)].astype(jnp.float32)
            + rbuf[RIGHT, half - 1, chunk(c)].astype(jnp.float32)
        )
        out[chunk(c), mine] = total.astype(jnp.bfloat16)
        for side in (LEFT, RIGHT):
            gather_copy(side, 0, c).start()
    for step in range(1, half):
        for k in range(CHUNKS):
            for side in (LEFT, RIGHT):
                c = (list(first[side]) + last[side])[k] if step >= half - 2 else k
                arrived(side, step - 1, c)
                if step < half - 1 or c in first[side]:
                    gather_copy(side, step, c).start()
    for side in (LEFT, RIGHT):
        for c in first[side]:
            arrived(side, half - 1, c)

    for side in (LEFT, RIGHT):
        for step in range(half):
            some = pl.ds(first[side][0] * cr, len(first[side]) * cr)
            part = some if step == 0 else pl.ds(0, rows)
            pltpu.make_async_remote_copy(
                src_ref=sbuf.at[side, step, part], dst_ref=rbuf.at[side, step, part],
                send_sem=send_sem.at[0, side, step], recv_sem=rs_sem.at[side, step, 0],
                device_id={AXIS: near[side]}, device_id_type=pl.DeviceIdType.MESH,
            ).wait_send()
            part = some if step == half - 1 else pl.ds(0, rows)
            ref = out.at[part, mine]
            pltpu.make_async_remote_copy(
                src_ref=ref, dst_ref=ref,
                send_sem=send_sem.at[1, side, step], recv_sem=ag_sem.at[side, step, 0],
                device_id={AXIS: near[side]}, device_id_type=pl.DeviceIdType.MESH,
            ).wait_send()


def solution(mesh):
    n = mesh.shape[AXIS]

    def step(x, w_gate, w_up, w_down):
        rows, model = x.shape
        depth = w_gate.shape[1]
        width, half = model // n, n // 2
        hbm = pl.BlockSpec(memory_space=pltpu.HBM)
        return pl.pallas_call(
            functools.partial(kernel, n),
            out_shape=jax.ShapeDtypeStruct((rows, model), jnp.bfloat16),
            in_specs=[hbm] * 4,
            out_specs=pl.BlockSpec(memory_space=pltpu.VMEM),
            scratch_shapes=[
                pltpu.VMEM((rows, model), jnp.bfloat16),
                pltpu.VMEM((SLOTS, model, SLAB), jnp.bfloat16),
                pltpu.VMEM((SLOTS, model, SLAB), jnp.bfloat16),
                pltpu.VMEM((n, depth, width), jnp.bfloat16),
                pltpu.VMEM((rows, depth), jnp.bfloat16),
                pltpu.VMEM((n, rows, width), jnp.float32),
                pltpu.VMEM((2, half, rows, width), jnp.bfloat16),
                pltpu.VMEM((2, half, rows, width), jnp.bfloat16),
                pltpu.SemaphoreType.DMA,
                pltpu.SemaphoreType.DMA((SLOTS,)),
                pltpu.SemaphoreType.DMA((SLOTS,)),
                pltpu.SemaphoreType.DMA((n,)),
                pltpu.SemaphoreType.DMA((2, 2, half)),
                pltpu.SemaphoreType.DMA((2, half, CHUNKS)),
                pltpu.SemaphoreType.DMA((2, half, CHUNKS)),
            ],
            compiler_params=pltpu.CompilerParams(
                collective_id=0, has_side_effects=True, vmem_limit_bytes=67_000_000
            ),
            cost_estimate=pl.CostEstimate(
                flops=6 * rows * model * depth, bytes_accessed=6 * model * depth, transcendentals=rows * depth
            ),
        )(x, w_gate, w_up, w_down)

    return jax.shard_map(
        step,
        mesh=mesh,
        in_specs=(P("dp", None), P(None, "tp"), P(None, "tp"), P("tp", None)),
        out_specs=P("dp", None),
        check_vma=False,
    )
```

```python
import contextlib
import functools

import jax
import jax.numpy as jnp
from jax import lax
from jax.experimental import pallas as pl
from jax.experimental.pallas import tpu as pltpu
from jax.sharding import PartitionSpec as P

AXIS = "tp"
SLAB = 256
SLOTS = 3
DOWN_SLOTS = 5
AHEAD = 3
BULK = 1
CHUNKS = 8
FIRST = 3
LEFT, RIGHT = 0, 1
PROFILE = False

ORDER = (
    0, 1001, 1107, 1000, 1106, 1105, 1002, 1103, 1104, 1, 1016, 1017, 1015, 2, 1111, 1014,
    1110, 1011, 1010, 1013, 1117, 1116, 1012, 3, 1115, 1026, 1114, 1027, 1112, 1025, 1113, 4,
    1121, 1021, 1020, 1024, 1120, 1127, 5, 1023, 1125, 1022, 1126, 6, 1124, 1123, 1037, 1122,
    1131, 1031, 1130, 1030, 1137, 1036, 1135, 1035, 1034, 1136, 7, 1134, 1033, 1133, 1032, 1132,
    2001, 2000, 2007, 2005, 2006, 2004, 2003, 2002, 3011, 3111, 3010, 3110, 3017, 3117, 3015, 3115,
    3016, 3116, 3014, 3114, 3013, 3113, 3012, 3112, 3021, 3121, 3020, 3120, 3027, 3127, 3025, 3125,
    3026, 3126, 3024, 3124, 3023, 3123, 3022, 3122, 3031, 3137, 3030, 3135, 3034, 3136, 3033, 3032,
)


def scope(name):
    return jax.named_scope(name) if PROFILE else contextlib.nullcontext()


def block_order(half):
    order = [half]
    for k in range(half - 1, 0, -1):
        order += [-k, k]
    return order + [0]


def offset_of(half, side, step):
    return (step - half if side == LEFT else half - step) if step else half


def decode(code):
    kind, rest = divmod(code, 1000)
    if kind == 0:
        return ("dot", rest)
    if kind == 2:
        return ("own", rest)
    return ("sum" if kind == 1 else "pass", rest // 100, rest // 10 % 10, rest % 10)


def plan(n):
    half = n // 2
    steps = [decode(code) for code in ORDER]
    first = {LEFT: range(FIRST), RIGHT: range(FIRST, CHUNKS)}

    def sent(op):
        if op[0] == "own":
            return [("pass", side, 0, op[1]) for side in (LEFT, RIGHT)]
        return [op] if op[0] in ("sum", "pass") else []

    def waited(op):
        if op[0] == "own":
            return [("sum", side, half - 1, op[1]) for side in (LEFT, RIGHT)]
        if op[0] == "pass":
            return [("pass", op[1], op[2] - 1, op[3])]
        if op[0] == "sum" and (op[2] > 1 or (op[2] == 1 and op[3] in first[op[1]])):
            return [("sum", op[1], op[2] - 1, op[3])]
        return []

    starts = {m: i for i, op in enumerate(steps) for m in sent(op)}
    ends = {m: i for i, op in enumerate(steps) for m in waited(op)}
    known = [dict.fromkeys(range(-half, half + 1), -1) for _ in steps]
    change = True
    while change:
        change = False
        for i, op in enumerate(steps):
            new = dict(known[i - 1]) if i else dict(known[0])
            new[0] = i
            for m in waited(op):
                away = 1 if m[1] == LEFT else -1
                for o, value in known[starts[m]].items():
                    if o + away in new:
                        new[o + away] = max(new[o + away], value)
            if new != known[i]:
                known[i], change = new, True
    semaphores, last = {}, []
    for m in sorted((m for m in starts if m in ends), key=lambda m: starts[m]):
        if m[0] == "sum" and m[2] == half - 1 and m[1] == RIGHT:
            continue
        pair = [m, ("sum", RIGHT, half - 1, m[3])] if m[0] == "sum" and m[2] == half - 1 else [m]
        for k, before in enumerate(last):
            if all(known[starts[x] - 1].get(-1 if x[1] == LEFT else 1, -1) >= before for x in pair):
                break
        else:
            k = len(last)
            last.append(None)
        last[k] = ends[m]
        for x in pair:
            semaphores[x] = k
    for m in starts:
        semaphores.setdefault(m, len(last))
    return steps, first, semaphores


def kernel(n, x_hbm, g_hbm, u_hbm, d_hbm, out, xb, gb, ub, wd, hid, early, term, sbuf, rbuf,
           x_sem, g_sem, u_sem, t_sem, d_sem, send_sem, recv_sem):
    rows, width = x_hbm.shape[0], d_hbm.shape[1] // n
    depth = g_hbm.shape[1]
    full, rest = depth // SLAB, depth % SLAB
    half = n // 2
    me = lax.axis_index(AXIS)
    near = {LEFT: lax.rem(me + n - 1, n), RIGHT: lax.rem(me + 1, n)}
    cr = rows // CHUNKS
    order = block_order(half)
    place = {o: b for b, o in enumerate(order)}
    steps, first, semaphores = plan(n)

    def at(offset):
        return lax.rem(me + offset + n, n)

    def slab(i):
        if isinstance(i, int) and i == 0 and rest:
            cols, size = pl.ds(full * SLAB, rest), rest
        else:
            cols, size = pl.ds(pl.multiple_of((i - lead) * SLAB, 128), SLAB), SLAB
        slot = i % SLOTS if isinstance(i, int) else lax.rem(i, SLOTS)
        dst = (slot, slice(None), pl.ds(0, size))
        return (
            pltpu.make_async_copy(g_hbm.at[:, cols], gb.at[dst], g_sem.at[slot]),
            pltpu.make_async_copy(u_hbm.at[:, cols], ub.at[dst], u_sem.at[slot]),
        )

    def parts(size, share):
        cut = int(size * share) // 256 * 256
        return pl.ds(0, cut), pl.ds(cut, size - cut)

    def final_slab():
        cols = pl.ds((full - 1) * SLAB, SLAB)
        slot = (slabs - 1) % SLOTS
        for k, part in enumerate(parts(x_hbm.shape[1], 0.5)):
            yield (
                part,
                pltpu.make_async_copy(g_hbm.at[part, cols], gb.at[slot, part], t_sem.at[0, k]),
                pltpu.make_async_copy(u_hbm.at[part, cols], ub.at[slot, part], t_sem.at[1, k]),
            )

    def down(b):
        cols = pl.ds(pl.multiple_of(at(order[b]) * width, 128), width)
        slot = b % DOWN_SLOTS
        pieces = parts(depth, 0.75) if b == 0 else [pl.ds(0, depth)]
        return [
            (part, pltpu.make_async_copy(d_hbm.at[part, cols], wd.at[slot, part], d_sem.at[DOWN_SLOTS if k else slot]))
            for k, part in enumerate(pieces)
        ]

    def start_down(b):
        for _, c in down(b):
            c.start(priority=BULK)

    lead = 1 if rest else 0
    slabs = full + lead
    x_copy = pltpu.make_async_copy(x_hbm, xb, x_sem)
    x_copy.start()
    for i in range(SLOTS):
        for c in slab(i):
            c.start()

    barrier = pltpu.get_barrier_semaphore()
    for side in (LEFT, RIGHT):
        pl.semaphore_signal(barrier, inc=1, device_id={AXIS: near[side]}, device_id_type=pl.DeviceIdType.MESH)

    with scope("xw"):
        x_copy.wait()

    def activate(gate, up):
        return (jax.nn.silu(gate) * up).astype(jnp.bfloat16)

    def dot(a, b):
        return jnp.dot(a, b, preferred_element_type=jnp.float32)

    if rest:
        for c in slab(0):
            c.wait()
        hid[:, full * SLAB :] = activate(dot(xb[...], gb[0, :, :rest]), dot(xb[...], ub[0, :, :rest]))
        for c in slab(SLOTS):
            c.start()

    @pl.loop(lead, slabs - 1)
    def _(i):
        slot = lax.rem(i, SLOTS)
        with scope("h"):
            for c in slab(i):
                c.wait()
            cols = pl.ds(pl.multiple_of((i - lead) * SLAB, 128), SLAB)
            hid[:, cols] = activate(dot(xb[...], gb[slot]), dot(xb[...], ub[slot]))

        @pl.when(i + SLOTS < slabs - 1)
        def _():
            for c in slab(i + SLOTS):
                c.start()

        @pl.when(i + SLOTS == slabs - 1)
        def _():
            for _, *both in final_slab():
                for c in both:
                    c.start()
            start_down(0)

        for b in range(1, AHEAD):
            @pl.when(i + SLOTS == slabs - 1 + b)
            def _():
                start_down(b)

    slot = (slabs - 1) % SLOTS
    for part, *both in final_slab():
        with scope("hw"):
            for c in both:
                c.wait()
        with scope("hr"):
            gate, up = dot(xb[:, part], gb[slot, part]), dot(xb[:, part], ub[slot, part])
            if part.start == 0:
                early[0], early[1] = gate, up
    with scope("hs"):
        hid[:, (full - 1) * SLAB : full * SLAB] = activate(early[0] + gate, early[1] + up)

    def chunk(c):
        return pl.ds(c * cr, cr)

    def remote(src, dst, sems, recv, side):
        return pltpu.make_async_remote_copy(
            src_ref=src,
            dst_ref=dst,
            send_sem=sems,
            recv_sem=recv,
            device_id={AXIS: near[side]},
            device_id_type=pl.DeviceIdType.MESH,
        )

    def sum_copy(side, step, c):
        return remote(
            sbuf.at[side, step, chunk(c)], rbuf.at[side, step, chunk(c)],
            send_sem, recv_sem.at[semaphores["sum", side, step, c]], side,
        )

    def columns(offset):
        return pl.ds(pl.multiple_of(at(offset) * width, 128), width)

    def pass_copy(side, step, c, hops=0):
        ref = out.at[chunk(c), columns(step + hops if side == LEFT else -step - hops)]
        return remote(ref, ref, send_sem, recv_sem.at[semaphores["pass", side, step, c]], side)

    met = False
    for op in steps:
        if op[0] == "dot":
            b = op[1]
            for k, (part, copy) in enumerate(down(b)):
                with scope(f"w{b}"):
                    copy.wait()
                if k == 0 and b + AHEAD < n:
                    start_down(b + AHEAD)
                with scope(f"d{b}"):
                    some = dot(hid[:, part], wd[b % DOWN_SLOTS, part])
                    term[b] = term[b] + some if k else some
        elif op[0] == "sum":
            _, side, step, c = op
            if not met:
                pl.semaphore_wait(barrier, 2)
                met = True
            total = term[place[offset_of(half, side, step)], chunk(c)]
            if step > 1 or (step == 1 and c in first[side]):
                with scope(f"r{side}{step}{c}"):
                    sum_copy(side, step - 1, c).wait_recv()
                total = total + rbuf[side, step - 1, chunk(c)].astype(jnp.float32)
            sbuf[side, step, chunk(c)] = total.astype(jnp.bfloat16)
            sum_copy(side, step, c).start()
        elif op[0] == "own":
            c = op[1]
            with scope(f"f{c}"):
                both = rbuf.at[:, half - 1, chunk(c)]
                remote(both, both, send_sem, recv_sem.at[semaphores["sum", LEFT, half - 1, c]], LEFT).wait_recv()
            total = term[place[0], chunk(c)]
            for side in (LEFT, RIGHT):
                total = total + rbuf[side, half - 1, chunk(c)].astype(jnp.float32)
            out[chunk(c), columns(0)] = total.astype(jnp.bfloat16)
            for side in (LEFT, RIGHT):
                pass_copy(side, 0, c).start()
        else:
            _, side, step, c = op
            with scope(f"a{side}{step}{c}"):
                pass_copy(side, step - 1, c, hops=1).wait_recv()
            pass_copy(side, step, c).start()

    with scope("z"):
        both = out.at[:, pl.ds(0, 2 * width)]
        remote(both, both, send_sem, recv_sem.at[max(semaphores.values())], LEFT).wait_recv()
    with scope("ws"):
        everything = term.at[pl.ds(0, n - 1)]
        remote(everything, everything, send_sem, recv_sem.at[0], LEFT).wait_send()


def solution(mesh):
    n = mesh.shape[AXIS]

    def step(x, w_gate, w_up, w_down):
        rows, model = x.shape
        depth = w_gate.shape[1]
        width, half = model // n, n // 2
        hbm = pl.BlockSpec(memory_space=pltpu.HBM)
        operands = [pltpu.with_memory_space_constraint(a, pltpu.HBM) for a in (x, w_gate, w_up, w_down)]
        return pl.pallas_call(
            functools.partial(kernel, n),
            out_shape=jax.ShapeDtypeStruct((rows, model), jnp.bfloat16),
            in_specs=[hbm] * 4,
            out_specs=pl.BlockSpec(memory_space=pltpu.VMEM),
            scratch_shapes=[
                pltpu.VMEM((rows, model), jnp.bfloat16),
                pltpu.VMEM((SLOTS, model, SLAB), jnp.bfloat16),
                pltpu.VMEM((SLOTS, model, SLAB), jnp.bfloat16),
                pltpu.VMEM((DOWN_SLOTS, depth, width), jnp.bfloat16),
                pltpu.VMEM((rows, depth), jnp.bfloat16),
                pltpu.VMEM((2, rows, SLAB), jnp.float32),
                pltpu.VMEM((n, rows, width), jnp.float32),
                pltpu.VMEM((2, half, rows, width), jnp.bfloat16),
                pltpu.VMEM((2, half, rows, width), jnp.bfloat16),
                pltpu.SemaphoreType.DMA,
                pltpu.SemaphoreType.DMA((SLOTS,)),
                pltpu.SemaphoreType.DMA((SLOTS,)),
                pltpu.SemaphoreType.DMA((2, 2)),
                pltpu.SemaphoreType.DMA((DOWN_SLOTS + 1,)),
                pltpu.SemaphoreType.DMA,
                pltpu.SemaphoreType.DMA((max(plan(n)[2].values()) + 1,)),
            ],
            compiler_params=pltpu.CompilerParams(
                collective_id=0, has_side_effects=True, vmem_limit_bytes=52_000_000
            ),
            cost_estimate=pl.CostEstimate(
                flops=6 * rows * model * depth, bytes_accessed=6 * model * depth, transcendentals=rows * depth
            ),
        )(*operands)

    return jax.shard_map(
        step,
        mesh=mesh,
        in_specs=(P("dp", None), P(None, "tp"), P(None, "tp"), P("tp", None)),
        out_specs=P("dp", None),
        check_vma=False,
    )
```

```python
import contextlib
import functools

import jax
import jax.numpy as jnp
from jax import lax
from jax.experimental import pallas as pl
from jax.experimental.pallas import tpu as pltpu
from jax.sharding import PartitionSpec as P

AXIS = "tp"
SLAB = 256
SLOTS = 3
DOWN_SLOTS = 5
AHEAD = 3
SPLIT = {0: 0.75, 2: 0.5}
BULK = 1
CHUNKS = 8
FIRST = 3
LEFT, RIGHT = 0, 1
PROFILE = False

ORDER = (
    0, 1001, 1107, 1000, 1106, 1105, 1002, 1103, 1104, 1, 1016, 1017, 1015, 2, 1111, 1014,
    1110, 1011, 1010, 1013, 1117, 1116, 1012, 3, 1115, 1026, 1114, 1027, 1112, 1025, 1113, 4,
    1121, 1021, 1020, 1024, 1120, 1127, 5, 1023, 1125, 1022, 1126, 6, 1124, 1123, 1037, 1122,
    1131, 1031, 1130, 1030, 1137, 1036, 1135, 1035, 1034, 1136, 7, 1134, 1033, 1133, 1032, 1132,
    2001, 2000, 2007, 2005, 2006, 2004, 2003, 2002, 3011, 3111, 3010, 3110, 3017, 3117, 3015, 3115,
    3016, 3116, 3014, 3114, 3013, 3113, 3012, 3112, 3021, 3121, 3020, 3120, 3027, 3127, 3025, 3125,
    3026, 3126, 3024, 3124, 3023, 3123, 3022, 3122, 3031, 3137, 3030, 3135, 3134, 3136, 3033, 3032,
)


def scope(name):
    return jax.named_scope(name) if PROFILE else contextlib.nullcontext()


def block_order(half):
    order = [half]
    for k in range(half - 1, 0, -1):
        order += [-k, k]
    return order + [0]


def offset_of(half, side, step):
    return (step - half if side == LEFT else half - step) if step else half


def decode(code):
    kind, rest = divmod(code, 1000)
    if kind == 0:
        return ("dot", rest)
    if kind == 2:
        return ("own", rest)
    return ("sum" if kind == 1 else "pass", rest // 100, rest // 10 % 10, rest % 10)


def plan(n):
    half = n // 2
    steps = [decode(code) for code in ORDER]
    first = {LEFT: range(FIRST), RIGHT: range(FIRST, CHUNKS)}

    def sent(op):
        if op[0] == "own":
            return [("pass", side, 0, op[1]) for side in (LEFT, RIGHT)]
        return [op] if op[0] in ("sum", "pass") else []

    def waited(op):
        if op[0] == "own":
            return [("sum", side, half - 1, op[1]) for side in (LEFT, RIGHT)]
        if op[0] == "pass":
            return [("pass", op[1], op[2] - 1, op[3])]
        if op[0] == "sum" and (op[2] > 1 or (op[2] == 1 and op[3] in first[op[1]])):
            return [("sum", op[1], op[2] - 1, op[3])]
        return []

    starts = {m: i for i, op in enumerate(steps) for m in sent(op)}
    ends = {m: i for i, op in enumerate(steps) for m in waited(op)}
    known = [dict.fromkeys(range(-half, half + 1), -1) for _ in steps]
    change = True
    while change:
        change = False
        for i, op in enumerate(steps):
            new = dict(known[i - 1]) if i else dict(known[0])
            new[0] = i
            for m in waited(op):
                away = 1 if m[1] == LEFT else -1
                for o, value in known[starts[m]].items():
                    if o + away in new:
                        new[o + away] = max(new[o + away], value)
            if new != known[i]:
                known[i], change = new, True
    semaphores, last = {}, []
    for m in sorted((m for m in starts if m in ends), key=lambda m: starts[m]):
        if m[0] == "sum" and m[2] == half - 1 and m[1] == RIGHT:
            continue
        pair = [m, ("sum", RIGHT, half - 1, m[3])] if m[0] == "sum" and m[2] == half - 1 else [m]
        for k, before in enumerate(last):
            if all(known[starts[x] - 1].get(-1 if x[1] == LEFT else 1, -1) >= before for x in pair):
                break
        else:
            k = len(last)
            last.append(None)
        last[k] = ends[m]
        for x in pair:
            semaphores[x] = k
    for m in starts:
        semaphores.setdefault(m, len(last))
    return steps, first, semaphores


def kernel(n, x_hbm, g_hbm, u_hbm, d_hbm, out, xb, gb, ub, wd, hid, early, term, sbuf, rbuf,
           x_sem, g_sem, u_sem, t_sem, d_sem, send_sem, recv_sem):
    rows, width = x_hbm.shape[0], d_hbm.shape[1] // n
    depth = g_hbm.shape[1]
    full, rest = depth // SLAB, depth % SLAB
    half = n // 2
    me = lax.axis_index(AXIS)
    near = {LEFT: lax.rem(me + n - 1, n), RIGHT: lax.rem(me + 1, n)}
    cr = rows // CHUNKS
    order = block_order(half)
    place = {o: b for b, o in enumerate(order)}
    steps, first, semaphores = plan(n)

    def at(offset):
        return lax.rem(me + offset + n, n)

    def slab(i):
        if isinstance(i, int) and i == 0 and rest:
            cols, size = pl.ds(full * SLAB, rest), rest
        else:
            cols, size = pl.ds(pl.multiple_of((i - lead) * SLAB, 128), SLAB), SLAB
        slot = i % SLOTS if isinstance(i, int) else lax.rem(i, SLOTS)
        dst = (slot, slice(None), pl.ds(0, size))
        return (
            pltpu.make_async_copy(g_hbm.at[:, cols], gb.at[dst], g_sem.at[slot]),
            pltpu.make_async_copy(u_hbm.at[:, cols], ub.at[dst], u_sem.at[slot]),
        )

    def parts(size, share):
        cut = int(size * share) // 256 * 256
        return pl.ds(0, cut), pl.ds(cut, size - cut)

    def final_slab():
        cols = pl.ds((full - 1) * SLAB, SLAB)
        slot = (slabs - 1) % SLOTS
        for k, part in enumerate(parts(x_hbm.shape[1], 0.5)):
            yield (
                part,
                pltpu.make_async_copy(g_hbm.at[part, cols], gb.at[slot, part], t_sem.at[0, k]),
                pltpu.make_async_copy(u_hbm.at[part, cols], ub.at[slot, part], t_sem.at[1, k]),
            )

    def down(b):
        cols = pl.ds(pl.multiple_of(at(order[b]) * width, 128), width)
        slot = b % DOWN_SLOTS
        pieces = parts(depth, SPLIT[b]) if b in SPLIT else [pl.ds(0, depth)]
        sems = [d_sem.at[slot]] + [d_sem.at[DOWN_SLOTS + i] for i, other in enumerate(SPLIT) if other == b]
        return [
            (part, pltpu.make_async_copy(d_hbm.at[part, cols], wd.at[slot, part], sem))
            for part, sem in zip(pieces, sems)
        ]

    def start_down(b):
        for _, c in down(b):
            c.start(priority=BULK)

    lead = 1 if rest else 0
    slabs = full + lead
    x_copy = pltpu.make_async_copy(x_hbm, xb, x_sem)
    x_copy.start()
    for i in range(SLOTS):
        for c in slab(i):
            c.start()

    barrier = pltpu.get_barrier_semaphore()
    for side in (LEFT, RIGHT):
        pl.semaphore_signal(barrier, inc=1, device_id={AXIS: near[side]}, device_id_type=pl.DeviceIdType.MESH)

    with scope("xw"):
        x_copy.wait()

    def activate(gate, up):
        return (jax.nn.silu(gate) * up).astype(jnp.bfloat16)

    def dot(a, b):
        return jnp.dot(a, b, preferred_element_type=jnp.float32)

    if rest:
        for c in slab(0):
            c.wait()
        hid[:, full * SLAB :] = activate(dot(xb[...], gb[0, :, :rest]), dot(xb[...], ub[0, :, :rest]))
        for c in slab(SLOTS):
            c.start()

    @pl.loop(lead, slabs - 1)
    def _(i):
        slot = lax.rem(i, SLOTS)
        with scope("h"):
            for c in slab(i):
                c.wait()
            cols = pl.ds(pl.multiple_of((i - lead) * SLAB, 128), SLAB)
            hid[:, cols] = activate(dot(xb[...], gb[slot]), dot(xb[...], ub[slot]))

        @pl.when(i + SLOTS < slabs - 1)
        def _():
            for c in slab(i + SLOTS):
                c.start()

        @pl.when(i + SLOTS == slabs - 1)
        def _():
            for _, *both in final_slab():
                for c in both:
                    c.start()
            start_down(0)

        for b in range(1, AHEAD):
            @pl.when(i + SLOTS == slabs - 1 + b)
            def _():
                start_down(b)

    slot = (slabs - 1) % SLOTS
    for part, *both in final_slab():
        with scope("hw"):
            for c in both:
                c.wait()
        with scope("hr"):
            gate, up = dot(xb[:, part], gb[slot, part]), dot(xb[:, part], ub[slot, part])
            if part.start == 0:
                early[0], early[1] = gate, up
    with scope("hs"):
        hid[:, (full - 1) * SLAB : full * SLAB] = activate(early[0] + gate, early[1] + up)

    def chunk(c):
        return pl.ds(c * cr, cr)

    def remote(src, dst, sems, recv, side):
        return pltpu.make_async_remote_copy(
            src_ref=src,
            dst_ref=dst,
            send_sem=sems,
            recv_sem=recv,
            device_id={AXIS: near[side]},
            device_id_type=pl.DeviceIdType.MESH,
        )

    def sum_copy(side, step, c):
        return remote(
            sbuf.at[side, step, chunk(c)], rbuf.at[side, step, chunk(c)],
            send_sem, recv_sem.at[semaphores["sum", side, step, c]], side,
        )

    def columns(offset):
        return pl.ds(pl.multiple_of(at(offset) * width, 128), width)

    def pass_copy(side, step, c, hops=0):
        ref = out.at[chunk(c), columns(step + hops if side == LEFT else -step - hops)]
        return remote(ref, ref, send_sem, recv_sem.at[semaphores["pass", side, step, c]], side)

    met = False
    for op in steps:
        if op[0] == "dot":
            b = op[1]
            for k, (part, copy) in enumerate(down(b)):
                with scope(f"w{b}"):
                    copy.wait()
                if k == 0 and b + AHEAD < n:
                    start_down(b + AHEAD)
                with scope(f"d{b}"):
                    some = dot(hid[:, part], wd[b % DOWN_SLOTS, part])
                    term[b] = term[b] + some if k else some
        elif op[0] == "sum":
            _, side, step, c = op
            if not met:
                pl.semaphore_wait(barrier, 2)
                met = True
            total = term[place[offset_of(half, side, step)], chunk(c)]
            if step > 1 or (step == 1 and c in first[side]):
                with scope(f"r{side}{step}{c}"):
                    sum_copy(side, step - 1, c).wait_recv()
                total = total + rbuf[side, step - 1, chunk(c)].astype(jnp.float32)
            sbuf[side, step, chunk(c)] = total.astype(jnp.bfloat16)
            sum_copy(side, step, c).start()
        elif op[0] == "own":
            c = op[1]
            with scope(f"f{c}"):
                both = rbuf.at[:, half - 1, chunk(c)]
                remote(both, both, send_sem, recv_sem.at[semaphores["sum", LEFT, half - 1, c]], LEFT).wait_recv()
            total = term[place[0], chunk(c)]
            for side in (LEFT, RIGHT):
                total = total + rbuf[side, half - 1, chunk(c)].astype(jnp.float32)
            out[chunk(c), columns(0)] = total.astype(jnp.bfloat16)
            for side in (LEFT, RIGHT):
                pass_copy(side, 0, c).start()
        else:
            _, side, step, c = op
            with scope(f"a{side}{step}{c}"):
                pass_copy(side, step - 1, c, hops=1).wait_recv()
            pass_copy(side, step, c).start()

    with scope("z"):
        both = out.at[:, pl.ds(0, 2 * width)]
        remote(both, both, send_sem, recv_sem.at[max(semaphores.values())], LEFT).wait_recv()
    with scope("ws"):
        everything = term.at[pl.ds(0, n - 1)]
        remote(everything, everything, send_sem, recv_sem.at[0], LEFT).wait_send()


def solution(mesh):
    n = mesh.shape[AXIS]

    def step(x, w_gate, w_up, w_down):
        rows, model = x.shape
        depth = w_gate.shape[1]
        width, half = model // n, n // 2
        hbm = pl.BlockSpec(memory_space=pltpu.HBM)
        operands = [pltpu.with_memory_space_constraint(a, pltpu.HBM) for a in (x, w_gate, w_up, w_down)]
        return pl.pallas_call(
            functools.partial(kernel, n),
            out_shape=jax.ShapeDtypeStruct((rows, model), jnp.bfloat16),
            in_specs=[hbm] * 4,
            out_specs=pl.BlockSpec(memory_space=pltpu.VMEM),
            scratch_shapes=[
                pltpu.VMEM((rows, model), jnp.bfloat16),
                pltpu.VMEM((SLOTS, model, SLAB), jnp.bfloat16),
                pltpu.VMEM((SLOTS, model, SLAB), jnp.bfloat16),
                pltpu.VMEM((DOWN_SLOTS, depth, width), jnp.bfloat16),
                pltpu.VMEM((rows, depth), jnp.bfloat16),
                pltpu.VMEM((2, rows, SLAB), jnp.float32),
                pltpu.VMEM((n, rows, width), jnp.float32),
                pltpu.VMEM((2, half, rows, width), jnp.bfloat16),
                pltpu.VMEM((2, half, rows, width), jnp.bfloat16),
                pltpu.SemaphoreType.DMA,
                pltpu.SemaphoreType.DMA((SLOTS,)),
                pltpu.SemaphoreType.DMA((SLOTS,)),
                pltpu.SemaphoreType.DMA((2, 2)),
                pltpu.SemaphoreType.DMA((DOWN_SLOTS + len(SPLIT),)),
                pltpu.SemaphoreType.DMA,
                pltpu.SemaphoreType.DMA((max(plan(n)[2].values()) + 1,)),
            ],
            compiler_params=pltpu.CompilerParams(
                collective_id=0, has_side_effects=True, vmem_limit_bytes=52_000_000
            ),
            cost_estimate=pl.CostEstimate(
                flops=6 * rows * model * depth, bytes_accessed=6 * model * depth, transcendentals=rows * depth
            ),
        )(*operands)

    return jax.shard_map(
        step,
        mesh=mesh,
        in_specs=(P("dp", None), P(None, "tp"), P(None, "tp"), P("tp", None)),
        out_specs=P("dp", None),
        check_vma=False,
    )
```

```python
import contextlib
import functools

import jax
import jax.numpy as jnp
from jax import lax
from jax.experimental import pallas as pl
from jax.experimental.pallas import tpu as pltpu
from jax.sharding import PartitionSpec as P

AXIS = "tp"
SLAB = 256
SLOTS = 3
DOWN_SLOTS = 5
AHEAD = 3
SPLIT = {0: 0.75, 1: 0.5, 2: 0.5}
BULK = 1
CHUNKS = 8
FIRST = 3
LEFT, RIGHT = 0, 1
PROFILE = False

ORDER = (
    0, 1001, 1105, 1107, 1106, 1104, 1000, 1002, 1, 1015, 1016, 1017, 1014, 1103, 2, 1111,
    1110, 1011, 1010, 1013, 1117, 1115, 1012, 1116, 3, 1114, 1025, 1112, 1113, 1026, 1027, 4,
    1121, 1021, 1020, 1024, 1120, 5, 1127, 1125, 1126, 1023, 6, 1124, 1022, 1122, 1123, 1037,
    1131, 1031, 1130, 1030, 1137, 1036, 1035, 1135, 7, 1136, 1134, 1034, 1033, 1133, 1132, 1032,
    2001, 2000, 2007, 2005, 2006, 2004, 2003, 2002, 3111, 3011, 3110, 3010, 3117, 3017, 3115, 3015,
    3116, 3014, 3114, 3013, 3012, 3113, 3016, 3112, 3121, 3020, 3021, 3127, 3027, 3125, 3024, 3126,
    3023, 3022, 3025, 3124, 3120, 3030, 3026, 3123, 3122, 3031, 3137, 3034, 3135, 3033, 3136, 3032,
)


def scope(name):
    return jax.named_scope(name) if PROFILE else contextlib.nullcontext()


def block_order(half):
    order = [half]
    for k in range(half - 1, 0, -1):
        order += [-k, k]
    return order + [0]


def offset_of(half, side, step):
    return (step - half if side == LEFT else half - step) if step else half


def decode(code):
    kind, rest = divmod(code, 1000)
    if kind == 0:
        return ("dot", rest)
    if kind == 2:
        return ("own", rest)
    return ("sum" if kind == 1 else "pass", rest // 100, rest // 10 % 10, rest % 10)


def plan(n):
    half = n // 2
    steps = [decode(code) for code in ORDER]
    first = {LEFT: range(FIRST), RIGHT: range(FIRST, CHUNKS)}

    def sent(op):
        if op[0] == "own":
            return [("pass", side, 0, op[1]) for side in (LEFT, RIGHT)]
        return [op] if op[0] in ("sum", "pass") else []

    def waited(op):
        if op[0] == "own":
            return [("sum", side, half - 1, op[1]) for side in (LEFT, RIGHT)]
        if op[0] == "pass":
            return [("pass", op[1], op[2] - 1, op[3])]
        if op[0] == "sum" and (op[2] > 1 or (op[2] == 1 and op[3] in first[op[1]])):
            return [("sum", op[1], op[2] - 1, op[3])]
        return []

    starts = {m: i for i, op in enumerate(steps) for m in sent(op)}
    ends = {m: i for i, op in enumerate(steps) for m in waited(op)}
    known = [dict.fromkeys(range(-half, half + 1), -1) for _ in steps]
    change = True
    while change:
        change = False
        for i, op in enumerate(steps):
            new = dict(known[i - 1]) if i else dict(known[0])
            new[0] = i
            for m in waited(op):
                away = 1 if m[1] == LEFT else -1
                for o, value in known[starts[m]].items():
                    if o + away in new:
                        new[o + away] = max(new[o + away], value)
            if new != known[i]:
                known[i], change = new, True
    semaphores, last = {}, []
    for m in sorted((m for m in starts if m in ends), key=lambda m: starts[m]):
        if m[0] == "sum" and m[2] == half - 1 and m[1] == RIGHT:
            continue
        pair = [m, ("sum", RIGHT, half - 1, m[3])] if m[0] == "sum" and m[2] == half - 1 else [m]
        for k, before in enumerate(last):
            if all(known[starts[x] - 1].get(-1 if x[1] == LEFT else 1, -1) >= before for x in pair):
                break
        else:
            k = len(last)
            last.append(None)
        last[k] = ends[m]
        for x in pair:
            semaphores[x] = k
    for m in starts:
        semaphores.setdefault(m, len(last))
    return steps, first, semaphores


def kernel(n, x_hbm, g_hbm, u_hbm, d_hbm, out, xb, gb, ub, wd, hid, early, term, sbuf, rbuf,
           x_sem, g_sem, u_sem, t_sem, d_sem, send_sem, recv_sem):
    rows, width = x_hbm.shape[0], d_hbm.shape[1] // n
    depth = g_hbm.shape[1]
    full, rest = depth // SLAB, depth % SLAB
    half = n // 2
    me = lax.axis_index(AXIS)
    near = {LEFT: lax.rem(me + n - 1, n), RIGHT: lax.rem(me + 1, n)}
    cr = rows // CHUNKS
    order = block_order(half)
    place = {o: b for b, o in enumerate(order)}
    steps, first, semaphores = plan(n)

    def at(offset):
        return lax.rem(me + offset + n, n)

    def slab(i):
        if isinstance(i, int) and i == 0 and rest:
            cols, size = pl.ds(full * SLAB, rest), rest
        else:
            cols, size = pl.ds(pl.multiple_of((i - lead) * SLAB, 128), SLAB), SLAB
        slot = i % SLOTS if isinstance(i, int) else lax.rem(i, SLOTS)
        dst = (slot, slice(None), pl.ds(0, size))
        return (
            pltpu.make_async_copy(g_hbm.at[:, cols], gb.at[dst], g_sem.at[slot]),
            pltpu.make_async_copy(u_hbm.at[:, cols], ub.at[dst], u_sem.at[slot]),
        )

    def parts(size, share):
        cut = int(size * share) // 256 * 256
        return pl.ds(0, cut), pl.ds(cut, size - cut)

    def final_slab():
        cols = pl.ds((full - 1) * SLAB, SLAB)
        slot = (slabs - 1) % SLOTS
        for k, part in enumerate(parts(x_hbm.shape[1], 0.5)):
            yield (
                part,
                pltpu.make_async_copy(g_hbm.at[part, cols], gb.at[slot, part], t_sem.at[0, k]),
                pltpu.make_async_copy(u_hbm.at[part, cols], ub.at[slot, part], t_sem.at[1, k]),
            )

    def down(b):
        cols = pl.ds(pl.multiple_of(at(order[b]) * width, 128), width)
        slot = b % DOWN_SLOTS
        pieces = parts(depth, SPLIT[b]) if b in SPLIT else [pl.ds(0, depth)]
        sems = [d_sem.at[slot]] + [d_sem.at[DOWN_SLOTS + i] for i, other in enumerate(SPLIT) if other == b]
        return [
            (part, pltpu.make_async_copy(d_hbm.at[part, cols], wd.at[slot, part], sem))
            for part, sem in zip(pieces, sems)
        ]

    def start_down(b):
        for _, c in down(b):
            c.start(priority=BULK)

    lead = 1 if rest else 0
    slabs = full + lead
    x_copy = pltpu.make_async_copy(x_hbm, xb, x_sem)
    x_copy.start()
    for i in range(SLOTS):
        for c in slab(i):
            c.start()

    barrier = pltpu.get_barrier_semaphore()
    for side in (LEFT, RIGHT):
        pl.semaphore_signal(barrier, inc=1, device_id={AXIS: near[side]}, device_id_type=pl.DeviceIdType.MESH)

    with scope("xw"):
        x_copy.wait()

    def activate(gate, up):
        return (jax.nn.silu(gate) * up).astype(jnp.bfloat16)

    def dot(a, b):
        return jnp.dot(a, b, preferred_element_type=jnp.float32)

    if rest:
        for c in slab(0):
            c.wait()
        hid[:, full * SLAB :] = activate(dot(xb[...], gb[0, :, :rest]), dot(xb[...], ub[0, :, :rest]))
        for c in slab(SLOTS):
            c.start()

    @pl.loop(lead, slabs - 1)
    def _(i):
        slot = lax.rem(i, SLOTS)
        with scope("h"):
            for c in slab(i):
                c.wait()
            cols = pl.ds(pl.multiple_of((i - lead) * SLAB, 128), SLAB)
            hid[:, cols] = activate(dot(xb[...], gb[slot]), dot(xb[...], ub[slot]))

        @pl.when(i + SLOTS < slabs - 1)
        def _():
            for c in slab(i + SLOTS):
                c.start()

        @pl.when(i + SLOTS == slabs - 1)
        def _():
            for _, *both in final_slab():
                for c in both:
                    c.start()
            start_down(0)

        for b in range(1, AHEAD):
            @pl.when(i + SLOTS == slabs - 1 + b)
            def _():
                start_down(b)

    slot = (slabs - 1) % SLOTS
    for part, *both in final_slab():
        with scope("hw"):
            for c in both:
                c.wait()
        with scope("hr"):
            gate, up = dot(xb[:, part], gb[slot, part]), dot(xb[:, part], ub[slot, part])
            if part.start == 0:
                early[0], early[1] = gate, up
    with scope("hs"):
        hid[:, (full - 1) * SLAB : full * SLAB] = activate(early[0] + gate, early[1] + up)

    def chunk(c):
        return pl.ds(c * cr, cr)

    def remote(src, dst, sems, recv, side):
        return pltpu.make_async_remote_copy(
            src_ref=src,
            dst_ref=dst,
            send_sem=sems,
            recv_sem=recv,
            device_id={AXIS: near[side]},
            device_id_type=pl.DeviceIdType.MESH,
        )

    def sum_copy(side, step, c):
        return remote(
            sbuf.at[side, step, chunk(c)], rbuf.at[side, step, chunk(c)],
            send_sem, recv_sem.at[semaphores["sum", side, step, c]], side,
        )

    def columns(offset):
        return pl.ds(pl.multiple_of(at(offset) * width, 128), width)

    def pass_copy(side, step, c, hops=0):
        ref = out.at[chunk(c), columns(step + hops if side == LEFT else -step - hops)]
        return remote(ref, ref, send_sem, recv_sem.at[semaphores["pass", side, step, c]], side)

    met = False
    for op in steps:
        if op[0] == "dot":
            b = op[1]
            for k, (part, copy) in enumerate(down(b)):
                with scope(f"w{b}"):
                    copy.wait()
                if k == 0 and b + AHEAD < n:
                    start_down(b + AHEAD)
                with scope(f"d{b}"):
                    some = dot(hid[:, part], wd[b % DOWN_SLOTS, part])
                    term[b] = term[b] + some if k else some
        elif op[0] == "sum":
            _, side, step, c = op
            if not met:
                pl.semaphore_wait(barrier, 2)
                met = True
            total = term[place[offset_of(half, side, step)], chunk(c)]
            if step > 1 or (step == 1 and c in first[side]):
                with scope(f"r{side}{step}{c}"):
                    sum_copy(side, step - 1, c).wait_recv()
                total = total + rbuf[side, step - 1, chunk(c)].astype(jnp.float32)
            sbuf[side, step, chunk(c)] = total.astype(jnp.bfloat16)
            sum_copy(side, step, c).start()
        elif op[0] == "own":
            c = op[1]
            with scope(f"f{c}"):
                both = rbuf.at[:, half - 1, chunk(c)]
                remote(both, both, send_sem, recv_sem.at[semaphores["sum", LEFT, half - 1, c]], LEFT).wait_recv()
            total = term[place[0], chunk(c)]
            for side in (LEFT, RIGHT):
                total = total + rbuf[side, half - 1, chunk(c)].astype(jnp.float32)
            out[chunk(c), columns(0)] = total.astype(jnp.bfloat16)
            for side in (LEFT, RIGHT):
                pass_copy(side, 0, c).start()
        else:
            _, side, step, c = op
            with scope(f"a{side}{step}{c}"):
                pass_copy(side, step - 1, c, hops=1).wait_recv()
            pass_copy(side, step, c).start()

    with scope("z"):
        both = out.at[:, pl.ds(0, 2 * width)]
        remote(both, both, send_sem, recv_sem.at[max(semaphores.values())], LEFT).wait_recv()
    with scope("ws"):
        everything = term.at[pl.ds(0, n - 1)]
        remote(everything, everything, send_sem, recv_sem.at[0], LEFT).wait_send()


def solution(mesh):
    n = mesh.shape[AXIS]

    def step(x, w_gate, w_up, w_down):
        rows, model = x.shape
        depth = w_gate.shape[1]
        width, half = model // n, n // 2
        hbm = pl.BlockSpec(memory_space=pltpu.HBM)
        operands = [pltpu.with_memory_space_constraint(a, pltpu.HBM) for a in (x, w_gate, w_up, w_down)]
        return pl.pallas_call(
            functools.partial(kernel, n),
            out_shape=jax.ShapeDtypeStruct((rows, model), jnp.bfloat16),
            in_specs=[hbm] * 4,
            out_specs=pl.BlockSpec(memory_space=pltpu.VMEM),
            scratch_shapes=[
                pltpu.VMEM((rows, model), jnp.bfloat16),
                pltpu.VMEM((SLOTS, model, SLAB), jnp.bfloat16),
                pltpu.VMEM((SLOTS, model, SLAB), jnp.bfloat16),
                pltpu.VMEM((DOWN_SLOTS, depth, width), jnp.bfloat16),
                pltpu.VMEM((rows, depth), jnp.bfloat16),
                pltpu.VMEM((2, rows, SLAB), jnp.float32),
                pltpu.VMEM((n, rows, width), jnp.float32),
                pltpu.VMEM((2, half, rows, width), jnp.bfloat16),
                pltpu.VMEM((2, half, rows, width), jnp.bfloat16),
                pltpu.SemaphoreType.DMA,
                pltpu.SemaphoreType.DMA((SLOTS,)),
                pltpu.SemaphoreType.DMA((SLOTS,)),
                pltpu.SemaphoreType.DMA((2, 2)),
                pltpu.SemaphoreType.DMA((DOWN_SLOTS + len(SPLIT),)),
                pltpu.SemaphoreType.DMA,
                pltpu.SemaphoreType.DMA((max(plan(n)[2].values()) + 1,)),
            ],
            compiler_params=pltpu.CompilerParams(
                collective_id=0, has_side_effects=True, vmem_limit_bytes=52_000_000
            ),
            cost_estimate=pl.CostEstimate(
                flops=6 * rows * model * depth, bytes_accessed=6 * model * depth, transcendentals=rows * depth
            ),
        )(*operands)

    return jax.shard_map(
        step,
        mesh=mesh,
        in_specs=(P("dp", None), P(None, "tp"), P(None, "tp"), P("tp", None)),
        out_specs=P("dp", None),
        check_vma=False,
    )
```

```python
import contextlib
import functools

import jax
import jax.numpy as jnp
from jax import lax
from jax.experimental import pallas as pl
from jax.experimental.pallas import tpu as pltpu
from jax.sharding import PartitionSpec as P

AXIS = "tp"
SLAB = 256
SLOTS = 3
DOWN_SLOTS = 5
AHEAD = 3
SPLIT = {0: 0.75, 2: 0.5}
BULK = 1
CHUNKS = 8
FIRST = 3
LEFT, RIGHT = 0, 1
PROFILE = False

ORDER = (
    0, 1001, 1107, 1000, 1106, 1105, 1002, 1103, 1104, 1, 1016, 1017, 1015, 2, 1111, 1014,
    1110, 1011, 1010, 1013, 1117, 1116, 1012, 3, 1115, 1026, 1114, 1027, 1112, 1025, 1113, 4,
    1121, 1021, 1020, 1024, 1120, 1127, 5, 1023, 1125, 1022, 1126, 6, 1124, 1123, 1037, 1122,
    1131, 1031, 1130, 1030, 1137, 1036, 1135, 1035, 1034, 1136, 7, 1134, 1033, 1133, 1032, 1132,
    2001, 2000, 2007, 2005, 2006, 2004, 2003, 2002, 3011, 3111, 3010, 3110, 3017, 3117, 3015, 3115,
    3016, 3116, 3014, 3114, 3013, 3113, 3012, 3112, 3021, 3121, 3020, 3120, 3027, 3127, 3025, 3125,
    3026, 3126, 3024, 3124, 3023, 3123, 3022, 3122, 3031, 3137, 3030, 3135, 3034, 3136, 3033, 3032,
)


def scope(name):
    return jax.named_scope(name) if PROFILE else contextlib.nullcontext()


def block_order(half):
    order = [half]
    for k in range(half - 1, 0, -1):
        order += [-k, k]
    return order + [0]


def offset_of(half, side, step):
    return (step - half if side == LEFT else half - step) if step else half


def decode(code):
    kind, rest = divmod(code, 1000)
    if kind == 0:
        return ("dot", rest)
    if kind == 2:
        return ("own", rest)
    return ("sum" if kind == 1 else "pass", rest // 100, rest // 10 % 10, rest % 10)


def plan(n):
    half = n // 2
    steps = [decode(code) for code in ORDER]
    first = {LEFT: range(FIRST), RIGHT: range(FIRST, CHUNKS)}

    def sent(op):
        if op[0] == "own":
            return [("pass", side, 0, op[1]) for side in (LEFT, RIGHT)]
        return [op] if op[0] in ("sum", "pass") else []

    def waited(op):
        if op[0] == "own":
            return [("sum", side, half - 1, op[1]) for side in (LEFT, RIGHT)]
        if op[0] == "pass":
            return [("pass", op[1], op[2] - 1, op[3])]
        if op[0] == "sum" and (op[2] > 1 or (op[2] == 1 and op[3] in first[op[1]])):
            return [("sum", op[1], op[2] - 1, op[3])]
        return []

    starts = {m: i for i, op in enumerate(steps) for m in sent(op)}
    ends = {m: i for i, op in enumerate(steps) for m in waited(op)}
    known = [dict.fromkeys(range(-half, half + 1), -1) for _ in steps]
    change = True
    while change:
        change = False
        for i, op in enumerate(steps):
            new = dict(known[i - 1]) if i else dict(known[0])
            new[0] = i
            for m in waited(op):
                away = 1 if m[1] == LEFT else -1
                for o, value in known[starts[m]].items():
                    if o + away in new:
                        new[o + away] = max(new[o + away], value)
            if new != known[i]:
                known[i], change = new, True
    semaphores, last = {}, []
    for m in sorted((m for m in starts if m in ends), key=lambda m: starts[m]):
        if m[0] == "sum" and m[2] == half - 1 and m[1] == RIGHT:
            continue
        pair = [m, ("sum", RIGHT, half - 1, m[3])] if m[0] == "sum" and m[2] == half - 1 else [m]
        for k, before in enumerate(last):
            if all(known[starts[x] - 1].get(-1 if x[1] == LEFT else 1, -1) >= before for x in pair):
                break
        else:
            k = len(last)
            last.append(None)
        last[k] = ends[m]
        for x in pair:
            semaphores[x] = k
    for m in starts:
        semaphores.setdefault(m, len(last))
    return steps, first, semaphores


def kernel(n, x_hbm, g_hbm, u_hbm, d_hbm, out, xb, gb, ub, wd, hid, early, term, sbuf, rbuf,
           x_sem, g_sem, u_sem, t_sem, d_sem, send_sem, recv_sem):
    rows, width = x_hbm.shape[0], d_hbm.shape[1] // n
    depth = g_hbm.shape[1]
    full, rest = depth // SLAB, depth % SLAB
    half = n // 2
    me = lax.axis_index(AXIS)
    near = {LEFT: lax.rem(me + n - 1, n), RIGHT: lax.rem(me + 1, n)}
    cr = rows // CHUNKS
    order = block_order(half)
    place = {o: b for b, o in enumerate(order)}
    steps, first, semaphores = plan(n)

    def at(offset):
        return lax.rem(me + offset + n, n)

    def slab(i):
        if isinstance(i, int) and i == 0 and rest:
            cols, size = pl.ds(full * SLAB, rest), rest
        else:
            cols, size = pl.ds(pl.multiple_of((i - lead) * SLAB, 128), SLAB), SLAB
        slot = i % SLOTS if isinstance(i, int) else lax.rem(i, SLOTS)
        dst = (slot, slice(None), pl.ds(0, size))
        return (
            pltpu.make_async_copy(g_hbm.at[:, cols], gb.at[dst], g_sem.at[slot]),
            pltpu.make_async_copy(u_hbm.at[:, cols], ub.at[dst], u_sem.at[slot]),
        )

    def parts(size, share):
        cut = int(size * share) // 256 * 256
        return pl.ds(0, cut), pl.ds(cut, size - cut)

    def final_slab():
        cols = pl.ds((full - 1) * SLAB, SLAB)
        slot = (slabs - 1) % SLOTS
        for k, part in enumerate(parts(x_hbm.shape[1], 0.5)):
            yield (
                part,
                pltpu.make_async_copy(g_hbm.at[part, cols], gb.at[slot, part], t_sem.at[0, k]),
                pltpu.make_async_copy(u_hbm.at[part, cols], ub.at[slot, part], t_sem.at[1, k]),
            )

    def down(b):
        cols = pl.ds(pl.multiple_of(at(order[b]) * width, 128), width)
        slot = b % DOWN_SLOTS
        pieces = parts(depth, SPLIT[b]) if b in SPLIT else [pl.ds(0, depth)]
        sems = [d_sem.at[slot]] + [d_sem.at[DOWN_SLOTS + i] for i, other in enumerate(SPLIT) if other == b]
        return [
            (part, pltpu.make_async_copy(d_hbm.at[part, cols], wd.at[slot, part], sem))
            for part, sem in zip(pieces, sems)
        ]

    def start_down(b):
        for _, c in down(b):
            c.start(priority=BULK)

    lead = 1 if rest else 0
    slabs = full + lead
    x_copy = pltpu.make_async_copy(x_hbm, xb, x_sem)
    x_copy.start()
    for i in range(SLOTS):
        for c in slab(i):
            c.start()

    barrier = pltpu.get_barrier_semaphore()
    for side in (LEFT, RIGHT):
        pl.semaphore_signal(barrier, inc=1, device_id={AXIS: near[side]}, device_id_type=pl.DeviceIdType.MESH)

    with scope("xw"):
        x_copy.wait()

    def activate(gate, up):
        return (jax.nn.silu(gate) * up).astype(jnp.bfloat16)

    def dot(a, b):
        return jnp.dot(a, b, preferred_element_type=jnp.float32)

    if rest:
        for c in slab(0):
            c.wait()
        hid[:, full * SLAB :] = activate(dot(xb[...], gb[0, :, :rest]), dot(xb[...], ub[0, :, :rest]))
        for c in slab(SLOTS):
            c.start()

    @pl.loop(lead, slabs - 1)
    def _(i):
        slot = lax.rem(i, SLOTS)
        with scope("h"):
            for c in slab(i):
                c.wait()
            cols = pl.ds(pl.multiple_of((i - lead) * SLAB, 128), SLAB)
            hid[:, cols] = activate(dot(xb[...], gb[slot]), dot(xb[...], ub[slot]))

        @pl.when(i + SLOTS < slabs - 1)
        def _():
            for c in slab(i + SLOTS):
                c.start()

        @pl.when(i + SLOTS == slabs - 1)
        def _():
            for _, *both in final_slab():
                for c in both:
                    c.start()
            start_down(0)

        for b in range(1, AHEAD):
            @pl.when(i + SLOTS == slabs - 1 + b)
            def _():
                start_down(b)

    slot = (slabs - 1) % SLOTS
    for part, *both in final_slab():
        with scope("hw"):
            for c in both:
                c.wait()
        with scope("hr"):
            gate, up = dot(xb[:, part], gb[slot, part]), dot(xb[:, part], ub[slot, part])
            if part.start == 0:
                early[0], early[1] = gate, up
    with scope("hs"):
        hid[:, (full - 1) * SLAB : full * SLAB] = activate(early[0] + gate, early[1] + up)

    def chunk(c):
        return pl.ds(c * cr, cr)

    def remote(src, dst, sems, recv, side):
        return pltpu.make_async_remote_copy(
            src_ref=src,
            dst_ref=dst,
            send_sem=sems,
            recv_sem=recv,
            device_id={AXIS: near[side]},
            device_id_type=pl.DeviceIdType.MESH,
        )

    def sum_copy(side, step, c):
        return remote(
            sbuf.at[side, step, chunk(c)], rbuf.at[side, step, chunk(c)],
            send_sem, recv_sem.at[semaphores["sum", side, step, c]], side,
        )

    def columns(offset):
        return pl.ds(pl.multiple_of(at(offset) * width, 128), width)

    def pass_copy(side, step, c, hops=0):
        ref = out.at[chunk(c), columns(step + hops if side == LEFT else -step - hops)]
        return remote(ref, ref, send_sem, recv_sem.at[semaphores["pass", side, step, c]], side)

    met = False
    for op in steps:
        if op[0] == "dot":
            b = op[1]
            for k, (part, copy) in enumerate(down(b)):
                with scope(f"w{b}"):
                    copy.wait()
                if k == 0 and b + AHEAD < n:
                    start_down(b + AHEAD)
                with scope(f"d{b}"):
                    some = dot(hid[:, part], wd[b % DOWN_SLOTS, part])
                    term[b] = term[b] + some if k else some
        elif op[0] == "sum":
            _, side, step, c = op
            if not met:
                pl.semaphore_wait(barrier, 2)
                met = True
            total = term[place[offset_of(half, side, step)], chunk(c)]
            if step > 1 or (step == 1 and c in first[side]):
                with scope(f"r{side}{step}{c}"):
                    sum_copy(side, step - 1, c).wait_recv()
                total = total + rbuf[side, step - 1, chunk(c)].astype(jnp.float32)
            sbuf[side, step, chunk(c)] = total.astype(jnp.bfloat16)
            sum_copy(side, step, c).start()
        elif op[0] == "own":
            c = op[1]
            with scope(f"f{c}"):
                both = rbuf.at[:, half - 1, chunk(c)]
                remote(both, both, send_sem, recv_sem.at[semaphores["sum", LEFT, half - 1, c]], LEFT).wait_recv()
            total = term[place[0], chunk(c)]
            for side in (LEFT, RIGHT):
                total = total + rbuf[side, half - 1, chunk(c)].astype(jnp.float32)
            out[chunk(c), columns(0)] = total.astype(jnp.bfloat16)
            for side in (LEFT, RIGHT):
                pass_copy(side, 0, c).start()
        else:
            _, side, step, c = op
            with scope(f"a{side}{step}{c}"):
                pass_copy(side, step - 1, c, hops=1).wait_recv()
            pass_copy(side, step, c).start()

    with scope("z"):
        both = out.at[:, pl.ds(0, 2 * width)]
        remote(both, both, send_sem, recv_sem.at[max(semaphores.values())], LEFT).wait_recv()
    with scope("ws"):
        everything = term.at[pl.ds(0, n - 1)]
        remote(everything, everything, send_sem, recv_sem.at[0], LEFT).wait_send()


def solution(mesh):
    n = mesh.shape[AXIS]

    def step(x, w_gate, w_up, w_down):
        rows, model = x.shape
        depth = w_gate.shape[1]
        width, half = model // n, n // 2
        hbm = pl.BlockSpec(memory_space=pltpu.HBM)
        operands = [pltpu.with_memory_space_constraint(a, pltpu.HBM) for a in (x, w_gate, w_up, w_down)]
        return pl.pallas_call(
            functools.partial(kernel, n),
            out_shape=jax.ShapeDtypeStruct((rows, model), jnp.bfloat16),
            in_specs=[hbm] * 4,
            out_specs=pl.BlockSpec(memory_space=pltpu.VMEM),
            scratch_shapes=[
                pltpu.VMEM((rows, model), jnp.bfloat16),
                pltpu.VMEM((SLOTS, model, SLAB), jnp.bfloat16),
                pltpu.VMEM((SLOTS, model, SLAB), jnp.bfloat16),
                pltpu.VMEM((DOWN_SLOTS, depth, width), jnp.bfloat16),
                pltpu.VMEM((rows, depth), jnp.bfloat16),
                pltpu.VMEM((2, rows, SLAB), jnp.float32),
                pltpu.VMEM((n, rows, width), jnp.float32),
                pltpu.VMEM((2, half, rows, width), jnp.bfloat16),
                pltpu.VMEM((2, half, rows, width), jnp.bfloat16),
                pltpu.SemaphoreType.DMA,
                pltpu.SemaphoreType.DMA((SLOTS,)),
                pltpu.SemaphoreType.DMA((SLOTS,)),
                pltpu.SemaphoreType.DMA((2, 2)),
                pltpu.SemaphoreType.DMA((DOWN_SLOTS + len(SPLIT),)),
                pltpu.SemaphoreType.DMA,
                pltpu.SemaphoreType.DMA((max(plan(n)[2].values()) + 1,)),
            ],
            compiler_params=pltpu.CompilerParams(
                collective_id=0, has_side_effects=True, vmem_limit_bytes=52_000_000
            ),
            cost_estimate=pl.CostEstimate(
                flops=6 * rows * model * depth, bytes_accessed=6 * model * depth, transcendentals=rows * depth
            ),
        )(*operands)

    return jax.shard_map(
        step,
        mesh=mesh,
        in_specs=(P("dp", None), P(None, "tp"), P(None, "tp"), P("tp", None)),
        out_specs=P("dp", None),
        check_vma=False,
    )
```
